32 devices in a mesh: cols: 8 (over y, x, core), rows: 4 (over z).
Axes of the slice: x: 2, y: 2, z: 4, core: 2. Of those that a mesh axis runs over, the one named last changes fastest.
Arguments:
- weight: float32 [8192, 28672], P('rows', 'cols'), may hold values from -6 to 6
- scales: float32 [8192], P('rows'), may hold values from 0.2 to 0.5
- panels: float32 [1024, 28672], P('cols', 'rows')
- block_inverse: float32 [2, 128, 128], replicated
- grid_codes: int32 [16], replicated, may hold values from -12 to 12, as said below
- block_starts: int32 [2], replicated, may hold values from 0 to 25088, as said below
Outputs:
- result: float32 [8192, 28672], P('rows', 'cols')
The draws below stay inside these ranges and needn't reach their ends.
Inputs may be any that keep to these rules, and one draw needn't show every extreme that they name: `grid_codes`: strictly increasing. `block_starts`: strictly increasing multiples of 3584; the last block starts at the last device's columns.
All inputs are finite; a program needn't handle non-finite values.
Results may differ from the reference program's by a relative error of at most 0.00012.
Values sent between devices are 32-bit elements; how exact they have to be, the bound alone decides.
A program may use at most 192 MiB of HBM per device.

```python
import math
import jax
import jax.numpy as jnp
from jax import lax

OUT = 8192
COLS_IN = 28672
BLK = 128
SUB = 32
LEVELS = 16
BLOCKS = 2
COLS_DEV = 3584
PANELS = 1024
N_COLS = 8


def draw_panels(key, part):
    row_ids = jnp.arange(PANELS, dtype=jnp.int32)[:, None]
    column_ids = jnp.arange(COLS_IN, dtype=jnp.int32)[None, :]
    start_col = row_ids // BLK * COLS_DEV
    local_row = row_ids % BLK
    inside = column_ids - start_col
    noise = jax.random.normal(jax.random.fold_in(key, 11), (PANELS, COLS_IN), jnp.float32)
    diag_vals = jnp.exp(jax.random.uniform(jax.random.fold_in(key, 12), (PANELS, COLS_IN), jnp.float32, -0.7, 0.7))
    upper = jnp.where(inside > local_row, noise / BLK ** 0.5, 0.0)
    upper = jnp.where(inside == local_row, diag_vals, upper)
    values = jnp.where(inside >= BLK, 2.0 * noise / BLK ** 0.5, upper)
    values = jnp.where(inside < 0, 0.0, values)
    return values.astype(jnp.float32)


def draw_block_inverse(key, part):
    noise = jax.random.normal(jax.random.fold_in(key, 21), (BLOCKS, BLK, BLK), jnp.float32)
    diag_vals = jax.random.uniform(jax.random.fold_in(key, 22), (BLOCKS, BLK, BLK), jnp.float32, 0.5, 1.5)
    row_ids = jnp.arange(BLK, dtype=jnp.int32)[:, None]
    column_ids = jnp.arange(BLK, dtype=jnp.int32)[None, :]
    values = jnp.where(column_ids > row_ids, 0.6 * noise / BLK ** 0.5, 0.0)
    values = jnp.where(column_ids == row_ids, diag_vals, values)
    return values.astype(jnp.float32)


def draw_grid_codes(key, part):
    picked = jax.random.permutation(jax.random.fold_in(key, 31), 25)[:LEVELS]
    return (jnp.sort(picked) - 12).astype(jnp.int32)


def draw_block_starts(key, part):
    earlier = jnp.sort(jax.random.permutation(jax.random.fold_in(key, 41), N_COLS - 1)[:BLOCKS - 1])
    owners = jnp.concatenate([earlier.astype(jnp.int32), jnp.full((1,), N_COLS - 1, jnp.int32)])
    return (owners * COLS_DEV).astype(jnp.int32)


def block_scale(rng, dims, cuts, low, high):
    gain, own = 1.0, jax.random.fold_in(rng, 6)
    for axis_at, blocks in cuts:
        draws = jnp.exp(jax.random.uniform(jax.random.fold_in(own, axis_at), (blocks,), jnp.float32, low / len(cuts), high / len(cuts)))
        gain = gain * jnp.repeat(draws, dims[axis_at] // blocks).reshape([-1 if axis == axis_at else 1 for axis in range(len(dims))])
    return gain


def normal_values(rng, dims, width, reach, split=(), kind=jnp.bfloat16):
    values = width * jax.random.normal(rng, dims, jnp.float32)
    if split:
        values = values * block_scale(rng, dims, split, -0.22, 0.18)
    return jnp.clip(values, -reach, reach).astype(kind)


def setup_inputs(seed: int = 0) -> dict:
    arg_keys = jax.random.split(jax.random.key(seed), 7)
    return {
        "weight": normal_values(arg_keys[0], (OUT, COLS_IN), 1.0, 6.0, ((0, 4), (1, 8)), jnp.float32),
        "scales": jnp.clip(jnp.exp(math.log(0.5) - 0.9162907 * jax.random.uniform(arg_keys[1], (OUT,), jnp.float32) ** block_scale(arg_keys[1], (OUT,), ((0, 4),), -0.2, 0.2)), 0.2, 0.5),
        "panels": draw_panels(jax.random.fold_in(arg_keys[6], 71), 0),
        "block_inverse": draw_block_inverse(jax.random.fold_in(arg_keys[6], 71), 0),
        "grid_codes": draw_grid_codes(jax.random.fold_in(arg_keys[6], 71), 0),
        "block_starts": draw_block_starts(jax.random.fold_in(arg_keys[6], 71), 0),
    }


softness = 0.2


def quantize(values, scales, grid_codes):
    levels = grid_codes.astype(jnp.float32)
    ratio = values / scales[:, None]
    output = jnp.zeros_like(values) + levels[0]
    for level_id in range(LEVELS - 1):
        level_gap = levels[level_id + 1] - levels[level_id]
        midpoint = 0.5 * (levels[level_id] + levels[level_id + 1])
        output = output + level_gap * jax.nn.sigmoid((ratio - midpoint) / softness)
    return output * scales[:, None]


def inner_block(block_cols, diag_block, inverse, scales, grid_codes):
    local_ids = jnp.arange(BLK, dtype=jnp.int32)
    pieces = []
    for piece_id in range(BLK // SUB):
        low_col = piece_id * SUB
        current = block_cols[:, low_col:low_col + SUB]
        quantized = quantize(current, scales, grid_codes)
        error_part = jnp.dot(current - quantized, inverse[low_col:low_col + SUB, low_col:low_col + SUB], precision=lax.Precision.HIGHEST, preferred_element_type=jnp.float32)
        later_rows = jnp.where(local_ids[None, :] >= low_col + SUB, diag_block[low_col:low_col + SUB, :], 0.0)
        block_cols = block_cols - jnp.dot(error_part, later_rows, precision=lax.Precision.HIGHEST, preferred_element_type=jnp.float32)
        block_cols = block_cols.at[:, low_col:low_col + SUB].set(quantized)
        pieces.append(error_part)
    return block_cols, jnp.concatenate(pieces, axis=1)


def reference(weight, scales, panels, block_inverse, grid_codes, block_starts):
    cols_per = COLS_IN // N_COLS
    column_ids = jnp.arange(COLS_IN, dtype=jnp.int32)
    for block_id in range(BLOCKS):
        start_col = block_starts[block_id].astype(jnp.int32)
        owner_id = (start_col // cols_per).astype(jnp.int32)
        panel_rows = lax.dynamic_slice_in_dim(panels, (owner_id * BLK).astype(jnp.int32), BLK, 0)
        diag_block = lax.dynamic_slice_in_dim(panel_rows, start_col, BLK, 1)
        block_cols = lax.dynamic_slice_in_dim(weight, start_col, BLK, 1)
        block_cols, errors = inner_block(block_cols, diag_block, block_inverse[block_id], scales, grid_codes)
        weight = lax.dynamic_update_slice_in_dim(weight, block_cols, start_col, 1)
        trail_rows = jnp.where(column_ids[None, :] >= start_col + BLK, panel_rows, 0.0)
        weight = weight - jnp.dot(errors, trail_rows, precision=lax.Precision.HIGHEST, preferred_element_type=jnp.float32)
    return weight
```

```python
import functools

import jax
import jax.numpy as jnp
from jax import lax
from jax.experimental import pallas as pl
from jax.experimental.pallas import tpu as pltpu
from jax.sharding import PartitionSpec as P

BLK = 128
SUB = 32
LEVELS = 16
BLOCKS = 2
GROUPS = BLK // SUB

softness = 0.2
F32, BF16 = jnp.float32, jnp.bfloat16


def split2(x):
    hi = x.astype(BF16)
    return hi, (x - hi.astype(F32)).astype(BF16)


def split3(x):
    hi = x.astype(BF16)
    rest = x - hi.astype(F32)
    mid = rest.astype(BF16)
    return hi, mid, (rest - mid.astype(F32)).astype(BF16)


def rounding_rows(inverse, diag_block):
    rows = lax.broadcasted_iota(jnp.int32, (BLK, BLK), 0) // SUB
    cols = lax.broadcasted_iota(jnp.int32, (BLK, BLK), 1) // SUB
    inv = jnp.where(rows == cols, inverse, 0.0)
    later = jnp.where(cols > rows, diag_block, 0.0)
    return inv + jnp.dot(
        inv, later, precision=lax.Precision.HIGHEST, preferred_element_type=F32
    )


def inner_block(block_t, scale, codes_ref, g_ref, base):
    levels = [codes_ref[k].astype(F32) for k in range(LEVELS)]
    sharp = 0.5 / softness
    center = 0.5 * (levels[0] + levels[LEVELS - 1])
    half = [0.5 * (levels[k + 1] - levels[k]) for k in range(LEVELS - 1)]
    mids = [sharp * 0.5 * (levels[k] + levels[k + 1]) for k in range(LEVELS - 1)]
    gain = sharp / scale
    groups = [block_t[j * SUB : (j + 1) * SUB, :] for j in range(GROUPS)]
    errors = []
    for j in range(GROUPS):
        current = groups[j]
        ratio = current * gain
        total = jnp.zeros_like(current) + center
        for k in range(LEVELS - 1):
            total = total + half[k] * jnp.tanh(ratio - mids[k])
        quantized = total * scale
        h, m, l = split3(current - quantized)
        stacked = jnp.concatenate([h, m, h, l, h, m, l, m], axis=0)
        moved = jnp.dot(g_ref[base + j], stacked, preferred_element_type=F32)
        errors.append(moved[j * SUB : (j + 1) * SUB, :])
        for i in range(j + 1, GROUPS):
            groups[i] = groups[i] - moved[i * SUB : (i + 1) * SUB, :]
        groups[j] = quantized
    return jnp.concatenate(groups, axis=0), jnp.concatenate(errors, axis=0)


def round_kernel(
    chunk, meta_ref, codes_ref, inv_ref, diag_ref, p0_ref, p1_ref, scale_ref, wblk_ref, w_ref, out_ref,
    pcat, gcat, ecat, block
):
    step = pl.program_id(0)
    cols_per = w_ref.shape[1]
    first = meta_ref[0]
    cut0, cut1 = meta_ref[1] + BLK, meta_ref[2] + BLK
    is_first = first == meta_ref[1]
    is_last = first == meta_ref[2]

    @pl.when(step == 0)
    def _():
        @pl.loop(0, cols_per // chunk)
        def _(i):
            at = pl.ds(pl.multiple_of(i * chunk, chunk), chunk)
            ids = first + i * chunk + lax.broadcasted_iota(jnp.int32, (BLK, chunk), 1)
            for b, (p_ref, cut) in enumerate(((p0_ref, cut0), (p1_ref, cut1))):
                hi, lo = split2(jnp.where(ids >= cut, p_ref[:, at], 0.0))
                pcat[b * BLK : (b + 1) * BLK, at] = hi
                pcat[(2 + b) * BLK : (3 + b) * BLK, at] = lo
                pcat[(4 + b) * BLK : (5 + b) * BLK, at] = hi

        for b in range(BLOCKS):
            diag = diag_ref[...] if b == 0 else p1_ref[:, :BLK]
            pieces = split3(rounding_rows(inv_ref[b], diag))
            h, m, l = [piece.astype(F32) for piece in pieces]
            for j in range(GROUPS):
                at = slice(j * SUB, (j + 1) * SUB)
                stacked = jnp.concatenate(
                    [h[at], h[at], m[at], h[at], l[at], m[at], m[at], l[at]], axis=0
                )
                gcat[b * GROUPS + j] = stacked.T.astype(BF16)
        ecat[...] = jnp.zeros_like(ecat)

    def put_errors(b, errors_t):
        hi, lo = split2(errors_t.T)
        ecat[:, b * BLK : (b + 1) * BLK] = hi
        ecat[:, (2 + b) * BLK : (3 + b) * BLK] = hi
        ecat[:, (4 + b) * BLK : (5 + b) * BLK] = lo

    scale = scale_ref[...]
    rounded, errors = inner_block(wblk_ref[...].T, scale, codes_ref, gcat, 0)
    put_errors(0, errors)
    block[...] = rounded

    @pl.when(is_last)
    def _():
        change = jnp.zeros((w_ref.shape[0], BLK), F32)
        for k in (0, 2, 4):
            at = slice(k * BLK, (k + 1) * BLK)
            change += jnp.dot(ecat[:, at], pcat[at, :BLK], preferred_element_type=F32)
        current = w_ref[:, :BLK] - change
        rounded, errors = inner_block(current.T, scale, codes_ref, gcat, GROUPS)
        put_errors(1, errors)
        block[...] = rounded

    @pl.loop(0, cols_per // chunk)
    def _(i):
        at = pl.ds(pl.multiple_of(i * chunk, chunk), chunk)
        out_ref[:, at] = w_ref[:, at] - jnp.dot(
            ecat[...], pcat[:, at], preferred_element_type=F32
        )

    @pl.when(jnp.logical_or(is_first, is_last))
    def _():
        out_ref[:, :BLK] = block[...].T


def round_local(meta, grid_codes, block_inverse, diag, p0, p1, scales, wblk, weight):
    rows, cols_per = weight.shape
    tile = next(t for t in (512, 256, 128, 64, 32, 16, 8) if rows % t == 0)
    chunk = next(c for c in (512, 256, 128) if cols_per % c == 0)
    smem = pl.BlockSpec(memory_space=pltpu.SMEM)

    def whole(shape):
        return pl.BlockSpec(shape, lambda i: (0,) * len(shape))

    return pl.pallas_call(
        functools.partial(round_kernel, chunk),
        grid=(rows // tile,),
        out_shape=jax.ShapeDtypeStruct(weight.shape, F32),
        in_specs=[
            smem,
            smem,
            whole((BLOCKS, BLK, BLK)),
            whole((BLK, BLK)),
            whole((BLK, cols_per)),
            whole((BLK, cols_per)),
            pl.BlockSpec((1, tile), lambda i: (0, i)),
            pl.BlockSpec((tile, BLK), lambda i: (i, 0)),
            pl.BlockSpec((tile, cols_per), lambda i: (i, 0)),
        ],
        out_specs=pl.BlockSpec((tile, cols_per), lambda i: (i, 0)),
        scratch_shapes=[
            pltpu.VMEM((6 * BLK, cols_per), BF16),
            pltpu.VMEM((BLOCKS * GROUPS, BLK, 8 * SUB), BF16),
            pltpu.VMEM((tile, 6 * BLK), BF16),
            pltpu.VMEM((BLK, tile), F32),
        ],
        compiler_params=pltpu.CompilerParams(
            dimension_semantics=("arbitrary",), vmem_limit_bytes=60 * 1024 * 1024
        ),
        name="round_local",
    )(meta, grid_codes, block_inverse, diag, p0, p1, scales[None, :], wblk, weight)


def local(weight, scales, panels, block_inverse, grid_codes, block_starts):
    cols_per = weight.shape[1]
    slab_width = panels.shape[1]
    own, row = lax.axis_index("cols"), lax.axis_index("rows")
    first = own * cols_per
    holder = first // slab_width
    offset = first - holder * slab_width
    start0, start1 = block_starts[0], block_starts[1]
    mine = own == start0 // cols_per
    slab, wblk = lax.psum(
        (jnp.where(mine, panels, 0.0), jnp.where(mine, weight[:, :BLK], 0.0)), "cols"
    )
    both = jnp.concatenate([slab, panels], axis=0)
    needed = lax.dynamic_slice_in_dim(both, offset, cols_per, 1)
    diag = lax.dynamic_slice_in_dim(slab, start0 % slab_width, BLK, 1)
    needed, diag = lax.psum(
        (jnp.where(row == holder, needed, 0.0), jnp.where(row == start0 // slab_width, diag, 0.0)), "rows"
    )
    meta = jnp.stack([first, start0, start1]).astype(jnp.int32)
    return round_local(
        meta, grid_codes, block_inverse, diag, needed[:BLK], needed[BLK:], scales, wblk, weight
    )


def solution(mesh):
    placed = (P("rows", "cols"), P("rows"), P("cols", "rows"), P(), P(), P())
    return jax.shard_map(
        local, mesh=mesh, in_specs=placed, out_specs=P("rows", "cols"), check_vma=False
    )
```

```python
import functools

import jax
import jax.numpy as jnp
from jax import lax
from jax.experimental import pallas as pl
from jax.experimental.pallas import tpu as pltpu
from jax.sharding import PartitionSpec as P

BLK = 128
SUB = 32
LEVELS = 16
BLOCKS = 2
GROUPS = BLK // SUB

softness = 0.2
F32, BF16 = jnp.float32, jnp.bfloat16
MESH = pl.DeviceIdType.MESH


def split2(x):
    hi = x.astype(BF16)
    return hi, (x - hi.astype(F32)).astype(BF16)


def split3(x):
    hi = x.astype(BF16)
    rest = x - hi.astype(F32)
    mid = rest.astype(BF16)
    return hi, mid, (rest - mid.astype(F32)).astype(BF16)


def rounding_rows(inverse, diag_block):
    rows = lax.broadcasted_iota(jnp.int32, (BLK, BLK), 0) // SUB
    cols = lax.broadcasted_iota(jnp.int32, (BLK, BLK), 1) // SUB
    inv = jnp.where(rows == cols, inverse, 0.0)
    later = jnp.where(cols > rows, diag_block, 0.0)
    return inv + jnp.dot(
        inv, later, precision=lax.Precision.HIGHEST, preferred_element_type=F32
    )


def inner_block(block_t, scale, codes_ref, g_ref, base):
    levels = [codes_ref[k].astype(F32) for k in range(LEVELS)]
    sharp = 0.5 / softness
    center = 0.5 * (levels[0] + levels[LEVELS - 1])
    half = [0.5 * (levels[k + 1] - levels[k]) for k in range(LEVELS - 1)]
    mids = [sharp * 0.5 * (levels[k] + levels[k + 1]) for k in range(LEVELS - 1)]
    gain = sharp / scale
    groups = [block_t[j * SUB : (j + 1) * SUB, :] for j in range(GROUPS)]
    errors = []
    for j in range(GROUPS):
        current = groups[j]
        ratio = current * gain
        total = jnp.zeros_like(current) + center
        for k in range(LEVELS - 1):
            total = total + half[k] * jnp.tanh(ratio - mids[k])
        quantized = total * scale
        h, m, l = split3(current - quantized)
        stacked = jnp.concatenate([h, m, h, l, h, m, l, m], axis=0)
        moved = jnp.dot(g_ref[base + j], stacked, preferred_element_type=F32)
        errors.append(moved[j * SUB : (j + 1) * SUB, :])
        for i in range(j + 1, GROUPS):
            groups[i] = groups[i] - moved[i * SUB : (i + 1) * SUB, :]
        groups[j] = quantized
    return jnp.concatenate(groups, axis=0), jnp.concatenate(errors, axis=0)


def round_kernel(
    chunk, meta_ref, codes_ref, inv_ref, diag_ref, p0_ref, p1_ref, scale_ref, wblk_ref, w_ref, out_ref,
    pcat, gcat, ecat, block
):
    step = pl.program_id(0)
    cols_per = w_ref.shape[1]
    first = meta_ref[0]
    cut0, cut1 = meta_ref[1] + BLK, meta_ref[2] + BLK
    is_first = first == meta_ref[1]
    is_last = first == meta_ref[2]

    @pl.when(step == 0)
    def _():
        @pl.loop(0, cols_per // chunk)
        def _(i):
            at = pl.ds(pl.multiple_of(i * chunk, chunk), chunk)
            ids = first + i * chunk + lax.broadcasted_iota(jnp.int32, (BLK, chunk), 1)
            for b, (p_ref, cut) in enumerate(((p0_ref, cut0), (p1_ref, cut1))):
                hi, lo = split2(jnp.where(ids >= cut, p_ref[:, at], 0.0))
                pcat[b * BLK : (b + 1) * BLK, at] = hi
                pcat[(2 + b) * BLK : (3 + b) * BLK, at] = lo
                pcat[(4 + b) * BLK : (5 + b) * BLK, at] = hi

        for b in range(BLOCKS):
            diag = diag_ref[...] if b == 0 else p1_ref[:, :BLK]
            pieces = split3(rounding_rows(inv_ref[b], diag))
            h, m, l = [piece.astype(F32) for piece in pieces]
            for j in range(GROUPS):
                at = slice(j * SUB, (j + 1) * SUB)
                stacked = jnp.concatenate(
                    [h[at], h[at], m[at], h[at], l[at], m[at], m[at], l[at]], axis=0
                )
                gcat[b * GROUPS + j] = stacked.T.astype(BF16)
        ecat[...] = jnp.zeros_like(ecat)

    def put_errors(b, errors_t):
        hi, lo = split2(errors_t.T)
        ecat[:, b * BLK : (b + 1) * BLK] = hi
        ecat[:, (2 + b) * BLK : (3 + b) * BLK] = hi
        ecat[:, (4 + b) * BLK : (5 + b) * BLK] = lo

    scale = scale_ref[...]
    rounded, errors = inner_block(wblk_ref[...].T, scale, codes_ref, gcat, 0)
    put_errors(0, errors)
    block[...] = rounded

    @pl.when(is_last)
    def _():
        change = jnp.zeros((w_ref.shape[0], BLK), F32)
        for k in (0, 2, 4):
            at = slice(k * BLK, (k + 1) * BLK)
            change += jnp.dot(ecat[:, at], pcat[at, :BLK], preferred_element_type=F32)
        current = w_ref[:, :BLK] - change
        rounded, errors = inner_block(current.T, scale, codes_ref, gcat, GROUPS)
        put_errors(1, errors)
        block[...] = rounded

    @pl.loop(0, cols_per // chunk)
    def _(i):
        at = pl.ds(pl.multiple_of(i * chunk, chunk), chunk)
        out_ref[:, at] = w_ref[:, at] - jnp.dot(
            ecat[...], pcat[:, at], preferred_element_type=F32
        )

    @pl.when(jnp.logical_or(is_first, is_last))
    def _():
        out_ref[:, :BLK] = block[...].T


def round_local(meta, grid_codes, block_inverse, diag, p0, p1, scales, wblk, weight):
    rows, cols_per = weight.shape
    tile = next(t for t in (512, 256, 128, 64, 32, 16, 8) if rows % t == 0)
    chunk = next(c for c in (512, 256, 128) if cols_per % c == 0)
    smem = pl.BlockSpec(memory_space=pltpu.SMEM)

    def whole(shape):
        return pl.BlockSpec(shape, lambda i: (0,) * len(shape))

    return pl.pallas_call(
        functools.partial(round_kernel, chunk),
        grid=(rows // tile,),
        out_shape=jax.ShapeDtypeStruct(weight.shape, F32),
        in_specs=[
            smem,
            smem,
            whole((BLOCKS, BLK, BLK)),
            whole((BLK, BLK)),
            whole((BLK, cols_per)),
            whole((BLK, cols_per)),
            pl.BlockSpec((1, tile), lambda i: (0, i)),
            pl.BlockSpec((tile, BLK), lambda i: (i, 0)),
            pl.BlockSpec((tile, cols_per), lambda i: (i, 0)),
        ],
        out_specs=pl.BlockSpec((tile, cols_per), lambda i: (i, 0)),
        scratch_shapes=[
            pltpu.VMEM((6 * BLK, cols_per), BF16),
            pltpu.VMEM((BLOCKS * GROUPS, BLK, 8 * SUB), BF16),
            pltpu.VMEM((tile, 6 * BLK), BF16),
            pltpu.VMEM((BLK, tile), F32),
        ],
        compiler_params=pltpu.CompilerParams(
            dimension_semantics=("arbitrary",), vmem_limit_bytes=60 * 1024 * 1024
        ),
        name="round_local",
    )(meta, grid_codes, block_inverse, diag, p0, p1, scales[None, :], wblk, weight)


def spread_kernel(
    pieces, ratio, last_only, with_diag, x_ref, d_ref, out_ref, dout_ref,
    held, slots, recv_sem, up_sem, down_sem, dsend_sem, drecv_sem
):
    rows, cols = lax.axis_size("rows"), lax.axis_size("cols")
    me, col = lax.axis_index("rows"), lax.axis_index("cols")
    holder = col // ratio
    depth = x_ref.shape[0] // pieces

    barrier = pltpu.get_barrier_semaphore()
    for step in range(1, rows):
        other = lax.rem(me + step, rows)
        pl.semaphore_signal(barrier, inc=1, device_id=(col, other), device_id_type=MESH)
    pl.semaphore_wait(barrier, rows - 1)

    def part(ref, i):
        return ref.at[pl.ds(i * depth, depth)]

    def copy(source, i, sems, target):
        return pltpu.make_async_remote_copy(
            src_ref=part(source, i),
            dst_ref=part(held, i),
            send_sem=sems.at[i],
            recv_sem=recv_sem.at[i],
            device_id=(col, target),
            device_id_type=MESH,
        )

    def diag_copy(step):
        other = lax.rem(me + step, rows)
        return pltpu.make_async_remote_copy(
            src_ref=d_ref,
            dst_ref=slots.at[step - 1],
            send_sem=dsend_sem.at[step - 1],
            recv_sem=drecv_sem.at[step - 1],
            device_id=(col, other),
            device_id_type=MESH,
        )

    if with_diag:
        for step in range(1, rows):
            diag_copy(step).start()

    active = col == cols - 1 if last_only else col >= 0
    goes_up = jnp.logical_and(me >= holder, me < rows - 1)
    goes_down = jnp.logical_and(me <= holder, me > 0)
    up = lax.rem(me + 1, rows)
    down = lax.rem(me + rows - 1, rows)

    @pl.when(active)
    def _():
        @pl.when(me == holder)
        def _():
            for i in range(pieces):
                @pl.when(goes_up)
                def _():
                    copy(x_ref, i, up_sem, up).start()

                @pl.when(goes_down)
                def _():
                    copy(x_ref, i, down_sem, down).start()

            out_ref[...] = x_ref[...]

        @pl.when(me != holder)
        def _():
            for i in range(pieces):
                copy(held, i, up_sem, up).wait_recv()

                @pl.when(goes_up)
                def _():
                    copy(held, i, up_sem, up).start()

                @pl.when(goes_down)
                def _():
                    copy(held, i, down_sem, down).start()

                at = slice(i * depth, (i + 1) * depth)
                out_ref[at, :] = held[at, :]

        for i in range(pieces):
            @pl.when(goes_up)
            def _():
                copy(held, i, up_sem, up).wait_send()

            @pl.when(goes_down)
            def _():
                copy(held, i, down_sem, down).wait_send()

    if last_only:
        @pl.when(jnp.logical_not(active))
        def _():
            out_ref[...] = x_ref[...]

    if with_diag:
        total = d_ref[...]
        for step in range(1, rows):
            diag_copy(step).wait()
            total = total + slots[step - 1]
        dout_ref[...] = total
    else:
        dout_ref[...] = d_ref[...]


def spread(x, diag, ratio, last_only, with_diag, collective_id):
    rows = lax.axis_size("rows")
    pieces = 16
    vmem = pl.BlockSpec(memory_space=pltpu.VMEM)
    sems = pltpu.SemaphoreType.DMA
    return pl.pallas_call(
        functools.partial(spread_kernel, pieces, ratio, last_only, with_diag),
        out_shape=(
            jax.ShapeDtypeStruct(x.shape, F32),
            jax.ShapeDtypeStruct(diag.shape, F32),
        ),
        in_specs=[vmem, vmem],
        out_specs=(vmem, vmem),
        scratch_shapes=[
            pltpu.VMEM(x.shape, F32),
            pltpu.VMEM((rows - 1,) + diag.shape, F32),
            sems((pieces,)),
            sems((pieces,)),
            sems((pieces,)),
            sems((rows - 1,)),
            sems((rows - 1,)),
        ],
        compiler_params=pltpu.CompilerParams(
            collective_id=collective_id, has_side_effects=True
        ),
        cost_estimate=pl.CostEstimate(
            flops=0, bytes_accessed=64 * x.size * 4, transcendentals=0
        ),
        name="spread",
    )(x, diag)


def local(weight, scales, panels, block_inverse, grid_codes, block_starts):
    cols_per = weight.shape[1]
    slab_width = panels.shape[1]
    own, row = lax.axis_index("cols"), lax.axis_index("rows")
    first = own * cols_per
    ratio = slab_width // cols_per
    offset = first % slab_width
    start0, start1 = block_starts[0], block_starts[1]
    mine = own == start0 // cols_per
    slab, wblk = lax.psum(
        (jnp.where(mine, panels, 0.0), jnp.where(mine, weight[:, :BLK], 0.0)), "cols"
    )
    none = jnp.zeros((8, BLK), F32)
    own1 = lax.dynamic_slice_in_dim(panels, offset, cols_per, 1)
    p1, _ = spread(own1, none, ratio, True, False, 1)
    own0 = lax.dynamic_slice_in_dim(slab, offset, cols_per, 1)
    diag = lax.dynamic_slice_in_dim(slab, start0 % slab_width, BLK, 1)
    diag = jnp.where(row == start0 // slab_width, diag, 0.0)
    p0, diag = spread(own0, diag, ratio, False, True, 2)
    meta = jnp.stack([first, start0, start1]).astype(jnp.int32)
    return round_local(meta, grid_codes, block_inverse, diag, p0, p1, scales, wblk, weight)


def solution(mesh):
    placed = (P("rows", "cols"), P("rows"), P("cols", "rows"), P(), P(), P())
    return jax.shard_map(
        local, mesh=mesh, in_specs=placed, out_specs=P("rows", "cols"), check_vma=False
    )
```
